128 devices in a mesh: seq: 16 (over z, x), tp: 8 (over y, core).
Axes of the slice: x: 4, y: 4, z: 4, core: 2. Of those that a mesh axis runs over, the one named last changes fastest.
Arguments:
- tokens: bfloat16 [2048, 6144], P('seq', 'tp'), may hold values from -6 to 6
- router_weight: bfloat16 [6144, 8], P('tp'), may hold values from -0.15625 to 0.15625
- expert_ids: int32 [2048, 2], P('seq'), may hold values from 0 to 7, all different within a row; in each aligned block of 128 rows (0 to 127, 128 to 255, ...) at most 56 rows name the same one
- gate_weight: bfloat16 [16, 6144, 4096], P('seq', None, 'tp'), may hold values from -0.078125 to 0.078125
- up_weight: bfloat16 [16, 6144, 4096], P('seq', None, 'tp'), may hold values from -0.078125 to 0.078125
- down_weight: bfloat16 [16, 4096, 6144], P('seq', 'tp'), may hold values from -0.0625 to 0.0625
Outputs:
- mixed: bfloat16 [2048, 6144], P('seq', 'tp')
The draws below stay inside these ranges and needn't reach their ends.
Inputs may be any that keep to these rules, and one draw needn't show every extreme that they name: `expert_ids`: each row names 2 different experts. In each aligned block of 128 rows (the tokens of one sequence group) no expert is named more than 56 times, a bound that some block reaches.
All inputs are finite; a program needn't handle non-finite values.
Results may differ from the reference program's by a relative error of at most 0.014.
Values may be sent and summed in bfloat16 or wider, within the bound.
No kernel may reach another device: no remote copies, remote signals or barrier semaphores. Data moves between devices by JAX's collectives and lax.ppermute only.
A program may use at most 128 MiB of HBM per device.

```python
import math
import jax
import jax.numpy as jnp
import numpy as np
from jax import lax

D = 6144
EXPERTS = 8
FF = 8192
TOP = 2
TOK_SEQ = 128
CAP = 56
SPLIT = 2
TOKENS = 2048
N_SEQ = 16
N_TP = 8


def steps_of(own_key, extent, shards, least, top_value):
    gain, own = 1.0, jax.random.fold_in(own_key, 6)
    for dim, parts in shards:
        steps = jnp.exp(jax.random.uniform(jax.random.fold_in(own, dim), (parts,), jnp.float32, least / len(shards), top_value / len(shards)))
        gain = gain * jnp.repeat(steps, extent[dim] // parts).reshape([-1 if axis == dim else 1 for axis in range(len(extent))])
    return gain


def shared_out(stream_key, own, number, rows, amount, top, limit, lean):
    order = jax.random.permutation(stream_key, amount)
    heavy_load, usual = load_shares(amount, rows * top, limit, lean, True), load_shares(amount, rows * top, limit, lean, False)
    places = jnp.arange(amount)

    def named(sizes, rotation):
        used = int((sizes > 0).sum())
        fixed = max(1, used // 4)
        passed = fixed + (places - fixed + rotation * (used - fixed)) % max(1, amount - fixed)
        return jnp.zeros((amount,), jnp.int32).at[order[jnp.where(places < fixed, places, passed)]].set(jnp.asarray(sizes, jnp.int32))

    sizes = jnp.where(number % 4 == 0, named(heavy_load, number // 4), named(usual, number - number // 4 - 1))
    mixed = jax.random.permutation(jax.random.fold_in(own, 3), amount)
    giver, taker = mixed[0:amount // 2 * 2:2], mixed[1:amount // 2 * 2:2]
    margin = jnp.minimum(sizes[giver] - 1, limit - sizes[taker]) // 2
    margin = jnp.where((giver == order[0]) | (taker == order[0]) | (sizes[taker] == 0), 0, jnp.maximum(margin, 0))
    passed = jax.random.randint(jax.random.fold_in(own, 4), (amount // 2,), 0, 1 << 20) % (margin + 1)
    sizes = sizes.at[giver].add(-passed).at[taker].add(passed)
    labels = jnp.searchsorted(jnp.cumsum(sizes), jnp.arange(rows * top), side="right").astype(jnp.int32)
    table = labels.reshape(top, rows).T
    table = table[jax.random.permutation(jax.random.fold_in(own, 1), rows)]
    rotation = jax.random.randint(jax.random.fold_in(own, 2), (rows, 1), 0, top)
    return jnp.take_along_axis(table, (jnp.arange(top)[None, :] + rotation) % top, axis=1)


def load_shares(number_of, total, reach, slope, full):
    loads = [(1 << 20) // math.isqrt(rank ** slope) + 1 for rank in range(1, number_of + 1)]
    largest = reach if full else min(reach, max(-(-total // number_of), total * loads[0] // sum(loads)))
    least = 1 if total - largest >= number_of - 1 else 0
    counts, surplus = [largest] + [least] * (number_of - 1), total - largest - least * (number_of - 1)
    while surplus > 0:
        movable = [i for i in range(1, number_of) if counts[i] < largest] or [i for i in range(1, number_of) if counts[i] < reach]
        whole, left = sum([loads[i] for i in movable]), surplus
        for i in movable:
            extra = min(reach - counts[i], max(1, left * loads[i] // whole), surplus)
            counts[i] = counts[i] + extra
            surplus = surplus - extra
    return np.array(counts)


def scatter_about(key, shape, spread, bound, pieces=(), held_as=jnp.bfloat16):
    entries = jax.random.normal(key, shape, jnp.float32) * spread
    if len(pieces) > 0:
        entries = steps_of(key, shape, pieces, -0.22, 0.18) * entries
    return jnp.clip(entries, min=-bound, max=bound).astype(held_as)


def setup_inputs(seed: int = 0) -> dict:
    streams_of = jax.random.split(jax.random.key(seed), 7)
    tokens = scatter_about(streams_of[0], (TOKENS, D), 1.0, 6.0, ((0, 16), (1, 8)))
    router_weight = scatter_about(streams_of[1], (D, EXPERTS), (D // 4) ** -0.5, 0.15625, ((0, 8),))
    expert_ids_keys = jax.random.split(jax.random.fold_in(streams_of[2], 1), TOKENS // TOK_SEQ)
    expert_ids_turns = jax.random.permutation(jax.random.fold_in(streams_of[2], 3), TOKENS // TOK_SEQ)
    expert_ids = jax.vmap(lambda own, number: shared_out(jax.random.fold_in(streams_of[2], 2), own, number, TOK_SEQ, EXPERTS, TOP, CAP, 2))(expert_ids_keys, expert_ids_turns).reshape((TOKENS, TOP))
    gate_weight = scatter_about(streams_of[3], (N_SEQ, D, FF // SPLIT), D ** -0.5, 0.078125, ((0, 16), (2, 8)))
    up_weight = scatter_about(streams_of[4], (N_SEQ, D, FF // SPLIT), D ** -0.5, 0.078125, ((0, 16), (2, 8)))
    down_weight = scatter_about(streams_of[5], (N_SEQ, FF // SPLIT, D), FF ** -0.5, 0.0625, ((0, 16), (1, 8)))
    return dict(tokens=tokens, router_weight=router_weight, expert_ids=expert_ids, gate_weight=gate_weight, up_weight=up_weight, down_weight=down_weight)


def reference(tokens, router_weight, expert_ids, gate_weight, up_weight, down_weight):
    halves = N_SEQ // EXPERTS
    block = FF // (halves * N_TP)
    logits = jnp.dot(tokens, router_weight, preferred_element_type=jnp.float32)
    chosen = expert_ids[:, :, None] == jnp.arange(EXPERTS, dtype=jnp.int32)[None, None, :]
    picked = jnp.sum(jnp.where(chosen, logits[:, None, :], jnp.float32(0.0)), axis=2)
    gates = jax.nn.sigmoid(picked - picked[:, ::-1])
    grouped = expert_ids.reshape(N_SEQ, TOK_SEQ * TOP)
    onehot = (grouped[:, :, None] == jnp.arange(EXPERTS, dtype=jnp.int32)[None, None, :]).astype(jnp.int32)
    before = jnp.cumsum(onehot, axis=1) - onehot
    slots = jnp.sum(before * onehot, axis=2).astype(jnp.int32)
    group_index = jnp.broadcast_to(jnp.arange(N_SEQ, dtype=jnp.int32)[:, None], grouped.shape)
    token_index = (group_index * TOK_SEQ + jnp.arange(TOK_SEQ * TOP, dtype=jnp.int32)[None, :] // TOP).astype(jnp.int32)
    table = jnp.full((EXPERTS, N_SEQ, CAP), TOKENS, jnp.int32).at[grouped, group_index, slots].set(token_index)
    padded = jnp.concatenate([tokens, jnp.zeros((1, D), tokens.dtype)], axis=0)

    def one_expert(expert):
        selected = padded[table[expert].reshape(-1)]
        total = jnp.zeros((N_SEQ * CAP, D), jnp.float32)
        for portion in range(halves):
            slab_index = expert * halves + portion
            gate_slab = gate_weight[slab_index]
            up_slab = up_weight[slab_index]
            down_slab = down_weight[slab_index]
            for shard in range(N_TP):
                low = shard * block
                gate = jnp.dot(selected, gate_slab[:, low:low + block], preferred_element_type=jnp.float32)
                up = jnp.dot(selected, up_slab[:, low:low + block], preferred_element_type=jnp.float32)
                hidden = (jax.nn.silu(gate) * up).astype(jnp.bfloat16)
                product = jnp.dot(hidden, down_slab[low:low + block, :], preferred_element_type=jnp.float32)
                rounded = lax.optimization_barrier(product.astype(jnp.bfloat16))
                total = total + rounded.astype(jnp.float32)
        return total

    outputs = lax.map(one_expert, jnp.arange(EXPERTS, dtype=jnp.int32))
    where_from = (grouped * (N_SEQ * CAP) + group_index * CAP + slots).astype(jnp.int32)
    gathered = outputs.reshape(EXPERTS * N_SEQ * CAP, D)[where_from.reshape(-1)].reshape(TOKENS, TOP, D)
    mixed = jnp.sum(gathered * gates[:, :, None], axis=1)
    return mixed.astype(jnp.bfloat16)
```

```python
import jax
import jax.numpy as jnp
from jax import lax
from jax.experimental import pallas as pl
from jax.experimental.pallas import tpu as pltpu
from jax.sharding import PartitionSpec as P


D = 6144
CAP = 56
BLK = 768
NEAR = ((0, 0), (0, 1), (0, 3), (0, 2), (1, 0), (3, 0), (2, 0))
FAR = ((1, 1), (1, 2), (1, 3), (2, 1), (2, 2), (2, 3), (3, 1), (3, 2), (3, 3))
RELS = (0, 3, 1, 2)
VMEM_SPEC = pl.BlockSpec(memory_space=pltpu.VMEM)
ANY_SPEC = pl.BlockSpec(memory_space=pl.ANY)
SMEM_SPEC = pl.BlockSpec(memory_space=pltpu.SMEM)


def f32(array):
    return array.astype(jnp.float32)


def bf16(array):
    return array.astype(jnp.bfloat16)


def dot(a, b):
    return jnp.dot(a, b, preferred_element_type=jnp.float32)


def in_vmem(array):
    return pltpu.with_memory_space_constraint(array, pltpu.VMEM)


def seq_shift(array, shift):
    dz, dx = shift
    if shift == (0, 0):
        return array
    pairs = []
    for place in range(16):
        z, x = divmod(place, 4)
        pairs.append((place, (z + dz) % 4 * 4 + (x + dx) % 4))
    return lax.ppermute(array, "seq", pairs)


def y_shift(array, step):
    pairs = [(2 * y + c, 2 * ((y + step) % 4) + c) for y in range(4) for c in range(2)]
    return lax.ppermute(array, "tp", pairs)


def core_swap(array):
    return lax.ppermute(array, "tp", [(p, p ^ 1) for p in range(8)])


def block_start(where, index):
    other, rel = divmod(index, 4)
    return pl.multiple_of((2 * ((where[0] + rel) % 4) + (where[1] + other) % 2) * BLK, BLK)


def gate_body(pieces, count, started, where, refs):
    xs, (gate_w, up_w), rest = refs[:count], refs[count : count + 2], refs[count + 2 :]
    if started:
        gin, uin, gacc, uacc = rest
    else:
        gacc, uacc = rest
    seen = set()
    for block, operand, lane, start, size in pieces:
        cut = pl.ds(block_start(where, block), BLK)
        x = xs[operand][:, lane : lane + BLK]
        rows = pl.ds(start, size)
        gate, up = dot(x, gate_w[cut, :]), dot(x, up_w[cut, :])
        if start in seen:
            gacc[rows, :] += gate
            uacc[rows, :] += up
        elif started:
            gacc[rows, :] = gin[rows, :] + gate
            uacc[rows, :] = uin[rows, :] + up
        else:
            gacc[rows, :] = gate
            uacc[rows, :] = up
        seen.add(start)


def cost(rows, ffn, share):
    return pl.CostEstimate(
        flops=int(6 * rows * D * ffn * share), transcendentals=rows * ffn, bytes_accessed=6 * D * ffn
    )


def gate_part(where, xs, pieces, rows, gate_slab, up_slab):
    ffn = gate_slab.shape[1]
    count = len(xs)

    def body(where, *refs):
        gate_body(pieces, count, False, where, refs)

    out = jax.ShapeDtypeStruct((rows, ffn), jnp.float32)
    return pl.pallas_call(
        body,
        out_shape=(out, out),
        in_specs=[SMEM_SPEC] + [VMEM_SPEC] * (count + 2),
        out_specs=(VMEM_SPEC, VMEM_SPEC),
        compiler_params=pltpu.CompilerParams(vmem_limit_bytes=16 * 1024 * 1024),
        cost_estimate=cost(rows, ffn, 0.5),
    )(where, *[in_vmem(x) for x in xs], gate_slab, up_slab)


def down_blocks(where, hid, down_w, target, first, obuf, sem):
    stores = []
    for rel in range(4):
        obuf[first + rel] = bf16(dot(hid, down_w[:, pl.ds(block_start(where, first + rel), BLK)]))
        copy = pltpu.make_async_copy(obuf.at[first + rel], target.at[rel], sem.at[first + rel])
        copy.start()
        stores.append(copy)
    return stores


def expert(where, xs, pieces, rows, gate_slab, up_slab, down_slab, sums, whole):
    ffn = gate_slab.shape[1]
    count = len(xs)

    def body(where, *refs):
        xs_w, refs = refs[: count + 2], refs[count + 2 :]
        down_w, given, refs = refs[0], refs[1:3], refs[3:]
        if whole:
            send, keep, gacc, uacc, hid, obuf, sem = refs
        else:
            send, hid, gacc, uacc, obuf, sem = refs
        gate_body(pieces, count, True, where, (*xs_w, *given, gacc, uacc))
        gate = gacc[...]
        hid[...] = bf16(gate / (1.0 + jnp.exp(-gate)) * uacc[...])
        stores = down_blocks(where, hid[...], down_w, send, 4, obuf, sem)
        if whole:
            stores = stores + down_blocks(where, hid[...], down_w, keep, 0, obuf, sem)
        for copy in stores:
            copy.wait()

    out = jax.ShapeDtypeStruct((4, rows, BLK), jnp.bfloat16)
    hidden = jax.ShapeDtypeStruct((rows, ffn), jnp.bfloat16)
    scratch = [pltpu.VMEM((rows, ffn), jnp.float32), pltpu.VMEM((rows, ffn), jnp.float32)]
    if whole:
        scratch.append(pltpu.VMEM((rows, ffn), jnp.bfloat16))
    return pl.pallas_call(
        body,
        out_shape=(out, out if whole else hidden),
        in_specs=[SMEM_SPEC] + [VMEM_SPEC] * (count + 5),
        out_specs=(ANY_SPEC, ANY_SPEC if whole else VMEM_SPEC),
        scratch_shapes=[
            *scratch,
            pltpu.VMEM((8, rows, BLK), jnp.bfloat16),
            pltpu.SemaphoreType.DMA((8,)),
        ],
        compiler_params=pltpu.CompilerParams(vmem_limit_bytes=20 * 1024 * 1024),
        cost_estimate=cost(rows, ffn, 0.5),
    )(
        where,
        *[in_vmem(x) for x in xs],
        gate_slab,
        up_slab,
        down_slab,
        *[in_vmem(a) for a in sums],
    )


def down_part(where, hid, down_slab):
    rows, ffn = hid.shape

    def body(where, hid, down_w, keep, obuf, sem):
        for copy in down_blocks(where, hid[...], down_w, keep, 0, obuf, sem):
            copy.wait()

    return pl.pallas_call(
        body,
        out_shape=jax.ShapeDtypeStruct((4, rows, BLK), jnp.bfloat16),
        in_specs=[SMEM_SPEC, VMEM_SPEC, VMEM_SPEC],
        out_specs=ANY_SPEC,
        scratch_shapes=[
            pltpu.VMEM((4, rows, BLK), jnp.bfloat16),
            pltpu.SemaphoreType.DMA((4,)),
        ],
        compiler_params=pltpu.CompilerParams(vmem_limit_bytes=10 * 1024 * 1024),
        cost_estimate=cost(rows, ffn, 0.2),
    )(where, in_vmem(hid), down_slab)


def placed(places, sources, picks, length):
    shape = sources[0].shape[-2:]
    count = len(sources)

    def value(places, index):
        return places[-1 - index] if index < 0 else index

    def body(places, *refs):
        ins, out = refs[:count], refs[count]
        for source, index, target in picks:
            ref = ins[source]
            block = ref[value(places, index)] if len(ref.shape) == 3 else ref[...]
            out[value(places, target)] = block

    return pl.pallas_call(
        body,
        out_shape=jax.ShapeDtypeStruct((length, *shape), sources[0].dtype),
        in_specs=[SMEM_SPEC] + [VMEM_SPEC] * count,
        out_specs=VMEM_SPEC,
        compiler_params=pltpu.CompilerParams(vmem_limit_bytes=10 * 1024 * 1024),
    )(places, *[in_vmem(a) for a in sources])


def resident(arrays):
    count = len(arrays)

    def body(*refs):
        ins, outs, sem = refs[:count], refs[count : 2 * count], refs[2 * count]
        copies = [pltpu.make_async_copy(a, b, sem.at[i]) for i, (a, b) in enumerate(zip(ins, outs))]
        for copy in copies:
            copy.start()
        for copy in copies:
            copy.wait()

    return pl.pallas_call(
        body,
        out_shape=tuple(pltpu.VMEM(a.shape, a.dtype) for a in arrays),
        in_specs=[pl.BlockSpec(memory_space=pltpu.HBM)] * count,
        out_specs=(VMEM_SPEC,) * count,
        scratch_shapes=[pltpu.SemaphoreType.DMA((count,))],
        compiler_params=pltpu.CompilerParams(vmem_limit_bytes=1024 * 1024),
    )(*[pltpu.with_memory_space_constraint(a, pltpu.HBM) for a in arrays])


def far_back(homes, base, first, second, length):
    count, rows, width = base.shape

    def body(homes, base, first, second, out):
        for i in range(length):
            if i < count:
                out[homes[i]] = bf16(base[i] + f32(first[i]) + f32(second[i]))
            else:
                out[homes[i]] = jnp.zeros((rows, width), jnp.bfloat16)

    return pl.pallas_call(
        body,
        out_shape=jax.ShapeDtypeStruct((length, rows, width), jnp.bfloat16),
        in_specs=[SMEM_SPEC] + [VMEM_SPEC] * 3,
        out_specs=VMEM_SPEC,
        compiler_params=pltpu.CompilerParams(vmem_limit_bytes=12 * 1024 * 1024),
    )(homes, *[in_vmem(a) for a in (base, first, second)])


def last_sum(base, parts, high, low, values):
    count = len(parts)

    def body(base, high, low, values, *refs):
        total = base[...] + dot(high[...], values[...]) + dot(low[...], values[...])
        for part in refs[:count]:
            total = total + f32(part[...])
        refs[count][...] = bf16(total)

    return pl.pallas_call(
        body,
        out_shape=jax.ShapeDtypeStruct(base.shape, jnp.bfloat16),
        in_specs=[VMEM_SPEC] * (4 + count),
        out_specs=VMEM_SPEC,
        compiler_params=pltpu.CompilerParams(vmem_limit_bytes=12 * 1024 * 1024),
    )(base, high, low, values, *parts)


def near_mix(high, low, values):
    count = len(values)
    tok_rows = high.shape[1]
    over_slots = (((0,), (0,)), ((), ()))

    def body(high, low, *refs):
        ins, first, others = refs[:count], refs[count], refs[count + 1]
        for rel in range(4):
            total = jnp.zeros((tok_rows, BLK), jnp.float32)
            for i in range(count):
                part = ins[i][rel]
                for weights in (high, low):
                    total = total + lax.dot_general(
                        weights[i * CAP : (i + 1) * CAP, :],
                        part,
                        over_slots,
                        preferred_element_type=jnp.float32,
                    )
            if rel == 0:
                first[...] = total
            else:
                others[rel - 1] = bf16(total)

    return pl.pallas_call(
        body,
        out_shape=(
            jax.ShapeDtypeStruct((tok_rows, BLK), jnp.float32),
            jax.ShapeDtypeStruct((3, tok_rows, BLK), jnp.bfloat16),
        ),
        in_specs=[VMEM_SPEC] * (2 + count),
        out_specs=(VMEM_SPEC, VMEM_SPEC),
        compiler_params=pltpu.CompilerParams(vmem_limit_bytes=16 * 1024 * 1024),
    )(high, low, *values)


def layer(tokens, router_weight, expert_ids, gate_weight, up_weight, down_weight):
    experts = router_weight.shape[1]
    tok_rows, top_count = expert_ids.shape
    here = lax.axis_index("seq")
    tp = lax.axis_index("tp")
    where = jnp.stack([tp // 2, tp % 2]).astype(jnp.int32)
    slabs = resident([w[0] for w in (gate_weight, up_weight, down_weight)])
    slabs = tuple(in_vmem(w) for w in slabs)
    z_here, x_here = here // 4, here % 4

    def place(shift, sign=1):
        return (z_here + sign * shift[0]) % 4 * 4 + (x_here + sign * shift[1]) % 4

    logits = dot(tokens, router_weight)
    terms = []
    rest = logits
    for _ in range(3):
        term = lax.reduce_precision(rest, 8, 7)
        terms.append(bf16(term))
        rest = rest - term
    pad = jnp.zeros((tok_rows, 128 - 3 * experts), jnp.bfloat16)
    packed = jnp.concatenate([tokens, jnp.concatenate(terms + [pad], axis=1)], axis=1)
    gathered = [packed] + [y_shift(packed, step) for step in (1, 3, 2)]

    flat_ids = expert_ids.reshape(-1)
    total = tok_rows * top_count
    onehot = flat_ids[:, None] == jnp.arange(experts, dtype=jnp.int32)[None, :]
    earlier = (
        jnp.arange(total, dtype=jnp.int32)[:, None] > jnp.arange(total, dtype=jnp.int32)[None, :]
    )
    before = dot(bf16(earlier), bf16(onehot))
    slots = jnp.sum(jnp.where(onehot, before, 0.0), axis=1).astype(jnp.int32)
    token_keys = expert_ids * CAP + slots.reshape(tok_rows, top_count)

    all_keys = jnp.arange(16 * CAP, dtype=jnp.int32)
    all_keys = all_keys // (2 * CAP) * CAP + all_keys % CAP
    matches = jnp.any(all_keys[:, None, None] == token_keys[None], axis=2)
    out = bf16(dot(bf16(matches), tokens)).reshape(16, CAP, BLK)
    received = lax.all_to_all(out, "seq", 0, 0, tiled=True)
    sources = jnp.stack([place(k, -1) for k in FAR]).astype(jnp.int32)
    count = len(FAR)
    far_rows = count * CAP
    own = placed(sources, [received], [(0, -1 - i, i) for i in range(count)], count)
    own = own.reshape(far_rows, BLK)

    full = jnp.concatenate([a[:, :BLK] for a in gathered], axis=1)
    slot_index = jnp.arange(CAP, dtype=jnp.int32)
    near_keys = jnp.stack([place(k) // 2 for k in NEAR])[:, None] * CAP + slot_index[None, :]
    matches = jnp.any(near_keys.reshape(-1)[:, None, None] == token_keys[None], axis=2)
    out = bf16(dot(bf16(matches), full))
    near = [seq_shift(out[i * CAP : (i + 1) * CAP], k) for i, k in enumerate(NEAR)]
    near_rows = len(NEAR) * CAP
    near_in = placed(where, near, [(i, 0, i) for i in range(len(NEAR))], len(NEAR))
    near_in = near_in.reshape(near_rows, 4 * BLK)
    near_other = core_swap(near_in)

    half_sum = jnp.zeros((tok_rows, experts), jnp.float32)
    for a in gathered:
        for i in range(3):
            half_sum = half_sum + f32(a[:, BLK + i * experts : BLK + (i + 1) * experts])
    logits = half_sum + core_swap(half_sum)
    chosen = expert_ids[:, :, None] == jnp.arange(experts, dtype=jnp.int32)[None, None, :]
    picked = jnp.sum(jnp.where(chosen, logits[:, None, :], 0.0), axis=2)
    gates = jax.nn.sigmoid(picked - picked[:, ::-1])

    def weights_of(keys):
        hit = token_keys[:, :, None] == keys[None, None, :]
        weights = jnp.sum(jnp.where(hit, gates[:, :, None], 0.0), axis=1)
        high = bf16(weights)
        return high, bf16(weights - f32(high))

    pieces = [(rel, 0, lane * BLK, 0, near_rows) for lane, rel in enumerate(RELS)]
    sums = gate_part(where, [near_in], pieces, near_rows, *slabs[:2])
    pieces = [(4 + rel, 0, lane * BLK, 0, near_rows) for lane, rel in enumerate(RELS)]
    send, keep = expert(where, [near_other], pieces, near_rows, *slabs, sums, True)
    got = core_swap(send)
    summed = bf16(f32(keep) + f32(got))
    returned = []
    for i, (dz, dx) in enumerate(NEAR):
        returned.append(seq_shift(summed[:, i * CAP : (i + 1) * CAP], ((-dz) % 4, (-dx) % 4)))
    hit = near_keys.reshape(-1)[:, None, None] == token_keys.T[None]
    weights = jnp.sum(jnp.where(hit, gates.T[None], 0.0), axis=1)
    high = bf16(weights)
    low = bf16(weights - f32(high))
    total, parts = near_mix(high, low, returned)
    summands = [y_shift(parts[rel - 1], rel) for rel in (1, 3, 2)]

    cut = far_rows // 32 * 16
    up1, dn1 = y_shift(own, 1), y_shift(own, 3)
    up2, dn2 = y_shift(up1[:cut], 1), y_shift(dn1[cut:], 3)
    first = [own, up1, dn1]
    first = first + [core_swap(a) for a in first]
    pieces = []
    for i, rel in enumerate((0, 3, 1)):
        pieces.append((rel, i, 0, 0, far_rows))
        pieces.append((4 + rel, 3 + i, 0, 0, far_rows))
    sums = gate_part(where, first, pieces, far_rows, *slabs[:2])
    last = [up2, dn2]
    last = last + [core_swap(a) for a in last]
    pieces = []
    for other in range(2):
        pieces.append((4 * other + 2, 2 * other, 0, 0, cut))
        pieces.append((4 * other + 2, 2 * other + 1, 0, cut, far_rows - cut))
    send, hid = expert(where, last, pieces, far_rows, *slabs, sums, False)
    got = core_swap(send)
    keep = down_part(where, hid, slabs[2])
    across_sum = bf16(f32(keep[2]) + f32(got[2]))
    from_below = y_shift(across_sum[:cut], 1)
    from_above = y_shift(across_sum[cut:], 3)
    zero_low = jnp.zeros((far_rows - cut, BLK), jnp.float32)
    zero_high = jnp.zeros((cut, BLK), jnp.float32)
    to_above = f32(keep[1]) + f32(got[1]) + jnp.concatenate([f32(from_below), zero_low], axis=0)
    to_below = f32(keep[3]) + f32(got[3]) + jnp.concatenate([zero_high, f32(from_above)], axis=0)
    shape = (count, CAP, BLK)
    homes = jnp.stack([place(k, -1) for k in FAR + NEAR]).astype(jnp.int32)
    base = (f32(keep[0]) + f32(got[0])).reshape(shape)
    from_below = y_shift(bf16(to_above), 1).reshape(shape)
    from_above = y_shift(bf16(to_below), 3).reshape(shape)
    back = far_back(homes, base, from_below, from_above, 16)
    values = lax.all_to_all(back, "seq", 0, 0, tiled=True).reshape(16 * CAP, BLK)
    seat = jnp.arange(16 * CAP, dtype=jnp.int32) // CAP
    is_far = (seat // 4 != z_here) & (seat % 4 != x_here)
    high, low = weights_of(jnp.where(is_far, all_keys, -1))
    return last_sum(total, summands, high, low, values)


def solution(mesh):
    in_specs = (
        P("seq", "tp"),
        P("tp", None),
        P("seq", None),
        P("seq", None, "tp"),
        P("seq", None, "tp"),
        P("seq", "tp", None),
    )
    out_specs = P("seq", "tp")
    return jax.shard_map(layer, mesh=mesh, in_specs=in_specs, out_specs=out_specs, check_vma=False)
```

```python
import jax
import jax.numpy as jnp
from jax import lax
from jax.experimental import pallas as pl
from jax.experimental.pallas import tpu as pltpu
from jax.sharding import PartitionSpec as P


D = 6144
CAP = 56
BLK = 768
NEAR = ((0, 0), (0, 1), (0, 3), (0, 2), (1, 0), (3, 0), (2, 0))
FAR = ((1, 1), (1, 2), (1, 3), (2, 1), (2, 2), (2, 3), (3, 1), (3, 2), (3, 3))
RELS = (0, 3, 1, 2)
VMEM_SPEC = pl.BlockSpec(memory_space=pltpu.VMEM)
ANY_SPEC = pl.BlockSpec(memory_space=pl.ANY)
SMEM_SPEC = pl.BlockSpec(memory_space=pltpu.SMEM)


def f32(array):
    return array.astype(jnp.float32)


def bf16(array):
    return array.astype(jnp.bfloat16)


def dot(a, b):
    return jnp.dot(a, b, preferred_element_type=jnp.float32)


def in_vmem(array):
    return pltpu.with_memory_space_constraint(array, pltpu.VMEM)


def seq_shift(array, shift):
    dz, dx = shift
    if shift == (0, 0):
        return array
    pairs = []
    for place in range(16):
        z, x = divmod(place, 4)
        pairs.append((place, (z + dz) % 4 * 4 + (x + dx) % 4))
    return lax.ppermute(array, "seq", pairs)


def y_shift(array, step):
    pairs = [(2 * y + c, 2 * ((y + step) % 4) + c) for y in range(4) for c in range(2)]
    return lax.ppermute(array, "tp", pairs)


def core_swap(array):
    return lax.ppermute(array, "tp", [(p, p ^ 1) for p in range(8)])


def block_start(where, index):
    other, rel = divmod(index, 4)
    return pl.multiple_of((2 * ((where[0] + rel) % 4) + (where[1] + other) % 2) * BLK, BLK)


def gate_body(pieces, count, started, where, refs):
    xs, (gate_w, up_w), rest = refs[:count], refs[count : count + 2], refs[count + 2 :]
    if started:
        gin, uin, gacc, uacc = rest
    else:
        gacc, uacc = rest
    seen = set()
    for block, operand, lane, start, size in pieces:
        cut = pl.ds(block_start(where, block), BLK)
        x = xs[operand][:, lane : lane + BLK]
        rows = pl.ds(start, size)
        gate, up = dot(x, gate_w[cut, :]), dot(x, up_w[cut, :])
        if start in seen:
            gacc[rows, :] += gate
            uacc[rows, :] += up
        elif started:
            gacc[rows, :] = gin[rows, :] + gate
            uacc[rows, :] = uin[rows, :] + up
        else:
            gacc[rows, :] = gate
            uacc[rows, :] = up
        seen.add(start)


def cost(rows, ffn, share):
    return pl.CostEstimate(
        flops=int(6 * rows * D * ffn * share), transcendentals=rows * ffn, bytes_accessed=6 * D * ffn
    )


def gate_part(where, xs, pieces, rows, gate_slab, up_slab):
    ffn = gate_slab.shape[1]
    count = len(xs)

    def body(where, *refs):
        gate_body(pieces, count, False, where, refs)

    out = jax.ShapeDtypeStruct((rows, ffn), jnp.float32)
    return pl.pallas_call(
        body,
        out_shape=(out, out),
        in_specs=[SMEM_SPEC] + [VMEM_SPEC] * (count + 2),
        out_specs=(VMEM_SPEC, VMEM_SPEC),
        compiler_params=pltpu.CompilerParams(vmem_limit_bytes=16 * 1024 * 1024),
        cost_estimate=cost(rows, ffn, 0.5),
    )(where, *[in_vmem(x) for x in xs], gate_slab, up_slab)


def down_blocks(where, hid, down_w, target, other, rels, obuf, sem, first=0):
    stores = []
    for i, rel in enumerate(rels):
        cut = pl.ds(block_start(where, 4 * other + rel), BLK)
        obuf[first + i] = bf16(dot(hid, down_w[:, cut]))
        copy = pltpu.make_async_copy(obuf.at[first + i], target.at[i], sem.at[first + i])
        copy.start()
        stores.append(copy)
    return stores


def expert(where, xs, pieces, rows, gate_slab, up_slab, down_slab, sums, rels, whole):
    ffn = gate_slab.shape[1]
    count = len(xs)
    width = len(rels)

    def body(where, *refs):
        xs_w, refs = refs[: count + 2], refs[count + 2 :]
        down_w, given, refs = refs[0], refs[1:3], refs[3:]
        if whole:
            send, keep, gacc, uacc, hid, obuf, sem = refs
        else:
            send, hid, gacc, uacc, obuf, sem = refs
        gate_body(pieces, count, True, where, (*xs_w, *given, gacc, uacc))
        gate = gacc[...]
        hid[...] = bf16(gate / (1.0 + jnp.exp(-gate)) * uacc[...])
        stores = down_blocks(where, hid[...], down_w, send, 1, rels, obuf, sem)
        if whole:
            stores = stores + down_blocks(where, hid[...], down_w, keep, 0, rels, obuf, sem, width)
        for copy in stores:
            copy.wait()

    out = jax.ShapeDtypeStruct((width, rows, BLK), jnp.bfloat16)
    hidden = jax.ShapeDtypeStruct((rows, ffn), jnp.bfloat16)
    scratch = [pltpu.VMEM((rows, ffn), jnp.float32), pltpu.VMEM((rows, ffn), jnp.float32)]
    if whole:
        scratch.append(pltpu.VMEM((rows, ffn), jnp.bfloat16))
    return pl.pallas_call(
        body,
        out_shape=(out, out if whole else hidden),
        in_specs=[SMEM_SPEC] + [VMEM_SPEC] * (count + 5),
        out_specs=(ANY_SPEC, ANY_SPEC if whole else VMEM_SPEC),
        scratch_shapes=[
            *scratch,
            pltpu.VMEM((2 * width, rows, BLK), jnp.bfloat16),
            pltpu.SemaphoreType.DMA((2 * width,)),
        ],
        compiler_params=pltpu.CompilerParams(vmem_limit_bytes=20 * 1024 * 1024),
        cost_estimate=cost(rows, ffn, 0.5),
    )(
        where,
        *[in_vmem(x) for x in xs],
        gate_slab,
        up_slab,
        down_slab,
        *[in_vmem(a) for a in sums],
    )


def down_part(where, hid, down_slab, other, rels):
    rows, ffn = hid.shape
    width = len(rels)

    def body(where, hid, down_w, out, obuf, sem):
        for copy in down_blocks(where, hid[...], down_w, out, other, rels, obuf, sem):
            copy.wait()

    return pl.pallas_call(
        body,
        out_shape=jax.ShapeDtypeStruct((width, rows, BLK), jnp.bfloat16),
        in_specs=[SMEM_SPEC, VMEM_SPEC, VMEM_SPEC],
        out_specs=ANY_SPEC,
        scratch_shapes=[
            pltpu.VMEM((width, rows, BLK), jnp.bfloat16),
            pltpu.SemaphoreType.DMA((width,)),
        ],
        compiler_params=pltpu.CompilerParams(vmem_limit_bytes=10 * 1024 * 1024),
        cost_estimate=cost(rows, ffn, 0.05 * width),
    )(where, in_vmem(hid), down_slab)


def placed(places, sources, picks, length):
    shape = sources[0].shape[-2:]
    count = len(sources)

    def value(places, index):
        return places[-1 - index] if index < 0 else index

    def body(places, *refs):
        ins, out = refs[:count], refs[count]
        for source, index, target in picks:
            ref = ins[source]
            block = ref[value(places, index)] if len(ref.shape) == 3 else ref[...]
            out[value(places, target)] = block

    return pl.pallas_call(
        body,
        out_shape=jax.ShapeDtypeStruct((length, *shape), sources[0].dtype),
        in_specs=[SMEM_SPEC] + [VMEM_SPEC] * count,
        out_specs=VMEM_SPEC,
        compiler_params=pltpu.CompilerParams(vmem_limit_bytes=10 * 1024 * 1024),
    )(places, *[in_vmem(a) for a in sources])


def resident(arrays):
    count = len(arrays)

    def body(*refs):
        ins, outs, sem = refs[:count], refs[count : 2 * count], refs[2 * count]
        copies = [pltpu.make_async_copy(a, b, sem.at[i]) for i, (a, b) in enumerate(zip(ins, outs))]
        for copy in copies:
            copy.start()
        for copy in copies:
            copy.wait()

    return pl.pallas_call(
        body,
        out_shape=tuple(pltpu.VMEM(a.shape, a.dtype) for a in arrays),
        in_specs=[pl.BlockSpec(memory_space=pltpu.HBM)] * count,
        out_specs=(VMEM_SPEC,) * count,
        scratch_shapes=[pltpu.SemaphoreType.DMA((count,))],
        compiler_params=pltpu.CompilerParams(vmem_limit_bytes=1024 * 1024),
    )(*[pltpu.with_memory_space_constraint(a, pltpu.HBM) for a in arrays])


def far_back(homes, base, first, second, length):
    count, rows, width = base.shape

    def body(homes, base, first, second, out):
        for i in range(length):
            if i < count:
                out[homes[i]] = bf16(base[i] + f32(first[i]) + f32(second[i]))
            else:
                out[homes[i]] = jnp.zeros((rows, width), jnp.bfloat16)

    return pl.pallas_call(
        body,
        out_shape=jax.ShapeDtypeStruct((length, rows, width), jnp.bfloat16),
        in_specs=[SMEM_SPEC] + [VMEM_SPEC] * 3,
        out_specs=VMEM_SPEC,
        compiler_params=pltpu.CompilerParams(vmem_limit_bytes=12 * 1024 * 1024),
    )(homes, *[in_vmem(a) for a in (base, first, second)])


def last_sum(base, parts, high, low, values):
    count = len(parts)

    def body(base, high, low, values, *refs):
        total = base[...] + dot(high[...], values[...]) + dot(low[...], values[...])
        for part in refs[:count]:
            total = total + f32(part[...])
        refs[count][...] = bf16(total)

    return pl.pallas_call(
        body,
        out_shape=jax.ShapeDtypeStruct(base.shape, jnp.bfloat16),
        in_specs=[VMEM_SPEC] * (4 + count),
        out_specs=VMEM_SPEC,
        compiler_params=pltpu.CompilerParams(vmem_limit_bytes=12 * 1024 * 1024),
    )(base, high, low, values, *parts)


def near_mix(high, low, values):
    count = len(values)
    tok_rows = high.shape[1]
    over_slots = (((0,), (0,)), ((), ()))

    def body(high, low, *refs):
        ins, first, others = refs[:count], refs[count], refs[count + 1]
        for rel in range(4):
            total = jnp.zeros((tok_rows, BLK), jnp.float32)
            for i in range(count):
                part = ins[i][rel]
                for weights in (high, low):
                    total = total + lax.dot_general(
                        weights[i * CAP : (i + 1) * CAP, :],
                        part,
                        over_slots,
                        preferred_element_type=jnp.float32,
                    )
            if rel == 0:
                first[...] = total
            else:
                others[rel - 1] = bf16(total)

    return pl.pallas_call(
        body,
        out_shape=(
            jax.ShapeDtypeStruct((tok_rows, BLK), jnp.float32),
            jax.ShapeDtypeStruct((3, tok_rows, BLK), jnp.bfloat16),
        ),
        in_specs=[VMEM_SPEC] * (2 + count),
        out_specs=(VMEM_SPEC, VMEM_SPEC),
        compiler_params=pltpu.CompilerParams(vmem_limit_bytes=16 * 1024 * 1024),
    )(high, low, *values)


def layer(tokens, router_weight, expert_ids, gate_weight, up_weight, down_weight):
    experts = router_weight.shape[1]
    tok_rows, top_count = expert_ids.shape
    here = lax.axis_index("seq")
    tp = lax.axis_index("tp")
    where = jnp.stack([tp // 2, tp % 2]).astype(jnp.int32)
    slabs = resident([w[0] for w in (gate_weight, up_weight, down_weight)])
    slabs = tuple(in_vmem(w) for w in slabs)
    z_here, x_here = here // 4, here % 4

    def place(shift, sign=1):
        return (z_here + sign * shift[0]) % 4 * 4 + (x_here + sign * shift[1]) % 4

    gathered = [tokens] + [y_shift(tokens, step) for step in (1, 3, 2)]
    partial = dot(tokens, router_weight)
    logits = partial
    for step in (1, 3, 2):
        logits = logits + y_shift(partial, step)

    flat_ids = expert_ids.reshape(-1)
    total = tok_rows * top_count
    onehot = flat_ids[:, None] == jnp.arange(experts, dtype=jnp.int32)[None, :]
    earlier = (
        jnp.arange(total, dtype=jnp.int32)[:, None] > jnp.arange(total, dtype=jnp.int32)[None, :]
    )
    before = dot(bf16(earlier), bf16(onehot))
    slots = jnp.sum(jnp.where(onehot, before, 0.0), axis=1).astype(jnp.int32)
    token_keys = expert_ids * CAP + slots.reshape(tok_rows, top_count)

    all_keys = jnp.arange(16 * CAP, dtype=jnp.int32)
    all_keys = all_keys // (2 * CAP) * CAP + all_keys % CAP
    matches = jnp.any(all_keys[:, None, None] == token_keys[None], axis=2)
    out = bf16(dot(bf16(matches), tokens)).reshape(16, CAP, BLK)
    received = lax.all_to_all(out, "seq", 0, 0, tiled=True)
    sources = jnp.stack([place(k, -1) for k in FAR]).astype(jnp.int32)
    count = len(FAR)
    far_rows = count * CAP
    own = placed(sources, [received], [(0, -1 - i, i) for i in range(count)], count)
    own = own.reshape(far_rows, BLK)

    full = jnp.concatenate(gathered, axis=1)
    slot_index = jnp.arange(CAP, dtype=jnp.int32)
    near_keys = jnp.stack([place(k) // 2 for k in NEAR])[:, None] * CAP + slot_index[None, :]
    matches = jnp.any(near_keys.reshape(-1)[:, None, None] == token_keys[None], axis=2)
    out = bf16(dot(bf16(matches), full))
    near = [seq_shift(out[i * CAP : (i + 1) * CAP], k) for i, k in enumerate(NEAR)]
    near_rows = len(NEAR) * CAP
    near_in = placed(where, near, [(i, 0, i) for i in range(len(NEAR))], len(NEAR))
    near_in = near_in.reshape(near_rows, 4 * BLK)
    near_other = core_swap(near_in)

    logits = logits + core_swap(logits)
    chosen = expert_ids[:, :, None] == jnp.arange(experts, dtype=jnp.int32)[None, None, :]
    picked = jnp.sum(jnp.where(chosen, logits[:, None, :], 0.0), axis=2)
    gates = jax.nn.sigmoid(picked - picked[:, ::-1])

    def weights_of(keys):
        hit = token_keys[:, :, None] == keys[None, None, :]
        weights = jnp.sum(jnp.where(hit, gates[:, :, None], 0.0), axis=1)
        high = bf16(weights)
        return high, bf16(weights - f32(high))

    pieces = [(rel, 0, lane * BLK, 0, near_rows) for lane, rel in enumerate(RELS)]
    sums = gate_part(where, [near_in], pieces, near_rows, *slabs[:2])
    pieces = [(4 + rel, 0, lane * BLK, 0, near_rows) for lane, rel in enumerate(RELS)]
    send, keep = expert(where, [near_other], pieces, near_rows, *slabs, sums, (0, 1, 2, 3), True)
    got = core_swap(send)
    summed = bf16(f32(keep) + f32(got))
    returned = []
    for i, (dz, dx) in enumerate(NEAR):
        returned.append(seq_shift(summed[:, i * CAP : (i + 1) * CAP], ((-dz) % 4, (-dx) % 4)))
    hit = near_keys.reshape(-1)[:, None, None] == token_keys.T[None]
    weights = jnp.sum(jnp.where(hit, gates.T[None], 0.0), axis=1)
    high = bf16(weights)
    low = bf16(weights - f32(high))
    total, parts = near_mix(high, low, returned)
    summands = [y_shift(parts[rel - 1], rel) for rel in (1, 3, 2)]

    cut = far_rows // 32 * 16
    up1, dn1 = y_shift(own, 1), y_shift(own, 3)
    up2, dn2 = y_shift(up1[:cut], 1), y_shift(dn1[cut:], 3)
    first = [own, up1, dn1]
    first = first + [core_swap(a) for a in first]
    pieces = []
    for i, rel in enumerate((0, 3, 1)):
        pieces.append((rel, i, 0, 0, far_rows))
        pieces.append((4 + rel, 3 + i, 0, 0, far_rows))
    sums = gate_part(where, first, pieces, far_rows, *slabs[:2])
    last = [up2, dn2]
    last = last + [core_swap(a) for a in last]
    pieces = []
    for other in range(2):
        pieces.append((4 * other + 2, 2 * other, 0, 0, cut))
        pieces.append((4 * other + 2, 2 * other + 1, 0, cut, far_rows - cut))
    send, hid = expert(where, last, pieces, far_rows, *slabs, sums, (2,), False)
    got = core_swap(send)
    keep = down_part(where, hid, slabs[2], 0, (2,))
    across_sum = bf16(f32(keep[0]) + f32(got[0]))
    send = down_part(where, hid, slabs[2], 1, (0, 1, 3))
    got = core_swap(send)
    keep = down_part(where, hid, slabs[2], 0, (0, 1, 3))
    from_below = y_shift(across_sum[:cut], 1)
    from_above = y_shift(across_sum[cut:], 3)
    zero_low = jnp.zeros((far_rows - cut, BLK), jnp.float32)
    zero_high = jnp.zeros((cut, BLK), jnp.float32)
    to_above = f32(keep[1]) + f32(got[1]) + jnp.concatenate([f32(from_below), zero_low], axis=0)
    to_below = f32(keep[2]) + f32(got[2]) + jnp.concatenate([zero_high, f32(from_above)], axis=0)
    shape = (count, CAP, BLK)
    homes = jnp.stack([place(k, -1) for k in FAR + NEAR]).astype(jnp.int32)
    base = (f32(keep[0]) + f32(got[0])).reshape(shape)
    from_below = y_shift(bf16(to_above), 1).reshape(shape)
    from_above = y_shift(bf16(to_below), 3).reshape(shape)
    back = far_back(homes, base, from_below, from_above, 16)
    values = lax.all_to_all(back, "seq", 0, 0, tiled=True).reshape(16 * CAP, BLK)
    seat = jnp.arange(16 * CAP, dtype=jnp.int32) // CAP
    is_far = (seat // 4 != z_here) & (seat % 4 != x_here)
    high, low = weights_of(jnp.where(is_far, all_keys, -1))
    return last_sum(total, summands, high, low, values)


def solution(mesh):
    in_specs = (
        P("seq", "tp"),
        P("tp", None),
        P("seq", None),
        P("seq", None, "tp"),
        P("seq", None, "tp"),
        P("seq", "tp", None),
    )
    out_specs = P("seq", "tp")
    return jax.shard_map(layer, mesh=mesh, in_specs=in_specs, out_specs=out_specs, check_vma=False)
```
